128 devices in a mesh: tasks: 1, group: 128 (over z, y, x, core).
Axes of the slice: x: 4, y: 4, z: 4, core: 2. Of those that a mesh axis runs over, the one named last changes fastest.
Arguments:
- points: bfloat16 [196608, 128], P(('tasks', 'group'))
- vectors: bfloat16 [196608, 64], P(('tasks', 'group'))
- lengthscale: float32 [1], replicated
- outscale: float32 [1], replicated
Outputs:
- output: float32 [196608, 64], P(('tasks', 'group'))
All inputs are finite; a program needn't handle non-finite values.
Results may differ from the reference program's by a relative error of at most 0.001.
Values are sent between devices in bfloat16 or wider.
A program may use at most 1 GiB of HBM per device.

```python
import jax
import jax.numpy as jnp
from jax import lax

NUM_POINTS = 196608
FEAT_DIM = 128
NUM_RHS = 64
QUERY_BLOCK = 256
LATENT_DIM = 8


def setup_inputs(seed: int = 0, part: int = 0) -> dict:
    base_key = jax.random.key(seed)
    part_key = jax.random.fold_in(base_key, part)
    key_lat, key_mix, key_noise, key_rhs = jax.random.split(part_key, 4)
    key_ell, key_scale = jax.random.split(jax.random.key(seed + 29), 2)
    latent = jax.random.normal(key_lat, (NUM_POINTS, LATENT_DIM), jnp.float32)
    mixing = jax.random.normal(key_mix, (LATENT_DIM, FEAT_DIM), jnp.float32) * FEAT_DIM ** -0.5
    noise = jax.random.normal(key_noise, (NUM_POINTS, FEAT_DIM), jnp.float32) * (0.3 * FEAT_DIM ** -0.5)
    points = (jnp.dot(latent, mixing) + noise).astype(jnp.bfloat16)
    vectors = (jax.random.normal(key_rhs, (NUM_POINTS, NUM_RHS), jnp.float32) * NUM_POINTS ** -0.5).astype(jnp.bfloat16)
    lengthscale = jax.random.uniform(key_ell, (1,), jnp.float32, 2.4, 3.1)
    outscale = jax.random.uniform(key_scale, (1,), jnp.float32, 0.6, 1.6)
    return {'points': points, 'vectors': vectors, 'lengthscale': lengthscale, 'outscale': outscale}


def reference(points, vectors, lengthscale, outscale):
    sq_norm = jnp.sum(jnp.square(points.astype(jnp.float32)), axis=1)
    two_ell_sq = 2.0 * jnp.square(lengthscale[0])
    query_pts = points.reshape(NUM_POINTS // QUERY_BLOCK, QUERY_BLOCK, FEAT_DIM)
    query_norm = sq_norm.reshape(NUM_POINTS // QUERY_BLOCK, QUERY_BLOCK)

    def one_block(block_pair):
        block_pts, block_norm = block_pair
        gram_mat = jnp.dot(block_pts, points.T, preferred_element_type=jnp.float32)
        sq_dist = jnp.maximum(block_norm[:, None] + sq_norm[None, :] - 2.0 * gram_mat, 0.0)
        kern_blk = (outscale[0] * jnp.exp(-sq_dist / two_ell_sq)).astype(jnp.bfloat16)
        return jnp.dot(kern_blk, vectors, preferred_element_type=jnp.float32)

    result = lax.map(one_block, (query_pts, query_norm))
    return result.reshape(NUM_POINTS, NUM_RHS)
```

```python
import functools

import jax
import jax.numpy as jnp
from jax import lax
from jax.experimental import pallas as pl
from jax.experimental.pallas import tpu as pltpu
from jax.sharding import PartitionSpec as P

OFFSETS = (0, 6, 7, 21, 26, 31, 33, 37, 49, 53, 73, 88, 96, 97)
ROWS = 1536
HALF = 768
TILE = 256
FEAT = 128
RHS = 64
F32 = jnp.float32
BF16 = jnp.bfloat16


def coords(g):
    return (g // 32, (g // 8) % 4, (g // 2) % 4, g % 2)


def difference(a, b):
    ca, cb = coords(a), coords(b)
    z, y, x = ((ca[k] - cb[k]) % 4 for k in range(3))
    return ((z * 4 + y) * 4 + x) * 2 + (ca[3] - cb[3]) % 2


def hops(g):
    return sum(min(v, 4 - v) for v in coords(g)[:3])


def make_plan():
    offsets = sorted(OFFSETS, key=lambda a: (hops(a), a))
    n_slots = len(offsets)
    units = [(0, 0, 6, 1), (0, 0, 7, 0)]
    seen = {0}
    for n in range(1, n_slots):
        first = True
        for m in range(n):
            g, back = difference(offsets[n], offsets[m]), difference(offsets[m], offsets[n])
            if g in seen:
                continue
            seen.update((g, back))
            if g == back:
                kinds = (2 + [k for k in range(4) if coords(g)[k]][0],)
            else:
                kinds = (0, 1)
            for kind in kinds:
                units.append((n, m, kind, 1 if first else 0))
                first = False
        assert not first
    assert len(seen) == 128
    last = {}
    for idx, (i, j, _, _) in enumerate(units):
        last[i] = idx
        last[j] = idx
    done = {}
    for slot, idx in last.items():
        if slot:
            done.setdefault(idx, []).append(slot)
    codes = []
    for idx, (i, j, kind, new) in enumerate(units):
        ready = done.get(idx, [])
        assert set(ready) <= {i, j}
        codes.append(i + 16 * j + 256 * kind + 2048 * new + 4096 * (i in ready) + 8192 * (j in ready and i != j))
    return offsets, codes


def pick(values, idx):
    out = jnp.int32(values[0])
    for k in range(1, len(values)):
        out = jnp.where(idx == k, jnp.int32(values[k]), out)
    return out


def kernel(offsets, codes, c_ref, s_ref, x_ref, v_ref, out_ref, xs, vts, xl, xt, yt, yrecv, kb, kt,
           xsend, vsend, xrecv, vrecv, ysend, ysem):
    n_slots = len(offsets)
    me = lax.axis_index('group')
    core, px, py, pz = me % 2, (me // 2) % 4, (me // 8) % 4, me // 32
    scale = c_ref[0]
    out_scale = s_ref[0]

    def shifted(z, y, x, c):
        return ((((pz + z) % 4) * 4 + (py + y) % 4) * 4 + (px + x) % 4) * 2 + (core + c) % 2

    def plus(a):
        return shifted(*coords(a))

    def minus(a):
        z, y, x, c = coords(a)
        return shifted((4 - z) % 4, (4 - y) % 4, (4 - x) % 4, c)

    partners = sorted(set(offsets[1:]) | {difference(0, a) for a in offsets[1:]})
    barrier = pltpu.get_barrier_semaphore()
    for a in partners:
        pl.semaphore_signal(barrier, inc=1, device_id=(0, plus(a)), device_id_type=pl.DeviceIdType.MESH)
    pl.semaphore_wait(barrier, len(partners))

    def x_copy(slot, target):
        return pltpu.make_async_remote_copy(
            src_ref=x_ref, dst_ref=xs.at[slot], send_sem=xsend.at[slot], recv_sem=xrecv.at[slot],
            device_id=(0, target), device_id_type=pl.DeviceIdType.MESH)

    def v_copy(slot, target):
        return pltpu.make_async_remote_copy(
            src_ref=v_ref, dst_ref=vts.at[slot], send_sem=vsend.at[slot], recv_sem=vrecv.at[slot],
            device_id=(0, target), device_id_type=pl.DeviceIdType.MESH)

    def y_copy(slot, target):
        return pltpu.make_async_remote_copy(
            src_ref=yt.at[slot], dst_ref=yrecv.at[slot], send_sem=ysend.at[slot], recv_sem=ysem.at[slot],
            device_id=(0, target), device_id_type=pl.DeviceIdType.MESH)

    for slot in range(1, n_slots):
        x_copy(slot, minus(offsets[slot])).start()
        v_copy(slot, minus(offsets[slot])).start()

    xs[0] = x_ref[...]
    vts[0] = v_ref[...]
    for slot in range(n_slots + 1):
        yt[slot] = jnp.zeros((RHS, ROWS), F32)

    lane = lax.broadcasted_iota(jnp.int32, (TILE, FEAT), 1)

    def prepare(slot):
        for t in range(ROWS // TILE):
            rows = slice(t * TILE, (t + 1) * TILE)
            x = xs[slot, rows, :]
            xf = x.astype(F32)
            norm = jnp.broadcast_to(jnp.sum(xf * xf, axis=1, keepdims=True), (TILE, FEAT))
            hi = norm.astype(BF16).astype(F32)
            mid = (norm - hi).astype(BF16).astype(F32)
            low = norm - hi - mid
            parts_at = lambda k: jnp.where(lane == k, hi, jnp.where(lane == k + 1, mid, low))
            left = jnp.where(lane < 3, 1.0, jnp.where(lane < 6, parts_at(3), 0.0)).astype(BF16)
            right = jnp.where(lane < 3, parts_at(0), jnp.where(lane < 6, 1.0, 0.0)).astype(BF16)
            xl[slot, rows, 0:FEAT] = x * BF16(-2.0)
            xl[slot, rows, FEAT:2 * FEAT] = left
            xt[slot, 0:FEAT, rows] = x.T
            xt[slot, FEAT:2 * FEAT, rows] = right.T

    def unit(i, j, h, y_i):
        start = pl.multiple_of(h * HALF, HALF)
        for jc in range(ROWS // TILE):
            cols = slice(jc * TILE, (jc + 1) * TILE)
            right = xt[j, :, cols]
            for ic in range(HALF // TILE):
                rows = slice(ic * TILE, (ic + 1) * TILE)
                left = xl[i, pl.ds(pl.multiple_of(start + ic * TILE, TILE), TILE), :]
                dist = jnp.maximum(jnp.dot(left, right, preferred_element_type=F32), 0.0)
                kern = (jnp.exp2(dist * scale) * out_scale).astype(BF16)
                kb[rows, cols] = kern
                kt[cols, rows] = kern.T
        v_i = vts[i, :, pl.ds(start, HALF)]
        for jc in range(ROWS // TILE):
            cols = slice(jc * TILE, (jc + 1) * TILE)
            yt[j, :, cols] += jnp.dot(v_i, kb[:, cols], preferred_element_type=F32)
        yt[y_i, :, pl.ds(start, HALF)] += jnp.dot(vts[j], kt[...], preferred_element_type=F32)

    def send_partial(slot):
        target = shifted(*(pick([coords(a)[k] for a in offsets], slot) for k in range(4)))
        y_copy(slot, target).start()

    per_word = 2
    words = [sum(code << (14 * r) for r, code in enumerate(codes[w:w + per_word]))
             for w in range(0, len(codes), per_word)]
    per_block = 6
    n_blocks = -(-len(words) // per_block)
    words += [0] * (n_blocks * per_block - len(words))

    def block(b, _):
        picked = [pick(words[r::per_block], b) for r in range(per_block)]
        count = jnp.minimum(len(codes) - b * (per_block * per_word), per_block * per_word)

        def step(q, ws):
            code = ws[0] % 16384
            odd = q % 2 == 1
            ws = tuple(jnp.where(odd, ws[r + 1] if r + 1 < per_block else 0, ws[r] if r else ws[0] // 16384)
                       for r in range(per_block))
            n, m, kind = code % 16, (code // 16) % 16, (code // 256) % 8
            new, done_i, done_j = (code // 2048) % 2, (code // 4096) % 2, (code // 8192) % 2
            bit = jnp.where(kind == 2, pz // 2, jnp.where(kind == 3, py // 2, jnp.where(kind == 4, px // 2, core)))
            shared = (kind >= 2) & (kind < 6)
            swap = shared & (bit == 1)
            i = jnp.where(swap, m, n)
            j = jnp.where(swap, n, m)
            h = jnp.where(shared, bit, kind % 2)
            y_i = jnp.where(kind >= 6, n_slots, i)

            @pl.when(new == 1)
            def _():
                @pl.when(n > 0)
                def _():
                    x_copy(n, me).wait_recv()
                    v_copy(n, me).wait_recv()
                prepare(n)

            unit(i, j, h, y_i)

            @pl.when(done_i == 1)
            def _():
                send_partial(n)

            @pl.when(done_j == 1)
            def _():
                send_partial(m)

            return ws

        lax.fori_loop(0, count, step, tuple(picked))
        return 0

    lax.fori_loop(0, n_blocks, block, 0)

    out_ref[...] = yt[0]
    for slot in range(1, n_slots):
        y_copy(slot, me).wait_recv()
        out_ref[...] += yrecv[slot]
    for slot in range(1, n_slots):
        x_copy(slot, me).wait_send()
        v_copy(slot, me).wait_send()
        y_copy(slot, me).wait_send()


def solution(mesh):
    row_spec = P(('tasks', 'group'), None)
    offsets, codes = make_plan()
    n_slots = len(offsets)

    def local_fn(x_loc, v_loc, lengthscale, outscale):
        scale = -1.4426950408889634 / (2.0 * jnp.square(lengthscale))
        smem = pl.BlockSpec(memory_space=pltpu.SMEM)
        vmem = pl.BlockSpec(memory_space=pltpu.VMEM)
        dma = pltpu.SemaphoreType.DMA((n_slots,))
        y_t = pl.pallas_call(
            functools.partial(kernel, offsets, codes),
            out_shape=jax.ShapeDtypeStruct((RHS, ROWS), F32),
            in_specs=[smem, smem, vmem, vmem],
            out_specs=vmem,
            scratch_shapes=[
                pltpu.VMEM((n_slots, ROWS, FEAT), BF16),
                pltpu.VMEM((n_slots, RHS, ROWS), BF16),
                pltpu.VMEM((n_slots, ROWS, 2 * FEAT), BF16),
                pltpu.VMEM((n_slots, 2 * FEAT, ROWS), BF16),
                pltpu.VMEM((n_slots + 1, RHS, ROWS), F32),
                pltpu.VMEM((n_slots, RHS, ROWS), F32),
                pltpu.VMEM((HALF, ROWS), BF16),
                pltpu.VMEM((ROWS, HALF), BF16),
                dma, dma, dma, dma, dma, dma,
            ],
            compiler_params=pltpu.CompilerParams(
                collective_id=0, has_side_effects=True, vmem_limit_bytes=60 * 1024 * 1024),
        )(scale, outscale, x_loc, v_loc.T)
        return y_t.T

    return jax.shard_map(local_fn, mesh=mesh, in_specs=(row_spec, row_spec, P(None), P(None)),
                         out_specs=row_spec, check_vma=False)
```

```python
import functools

import jax
import jax.numpy as jnp
from jax import lax
from jax.experimental import pallas as pl
from jax.experimental.pallas import tpu as pltpu
from jax.sharding import PartitionSpec as P

OFFSETS = (0, 6, 7, 21, 26, 31, 33, 37, 49, 53, 73, 88, 96, 97)
ROWS = 1536
HALF = 768
UNROLL = 3
LAG = 8
STEPS = 18
PANEL = 128
TILE = 256
FEAT = 128
RHS = 64
F32 = jnp.float32
BF16 = jnp.bfloat16


def coords(g):
    return (g // 32, (g // 8) % 4, (g // 2) % 4, g % 2)


def difference(a, b):
    ca, cb = coords(a), coords(b)
    z, y, x = ((ca[k] - cb[k]) % 4 for k in range(3))
    return ((z * 4 + y) * 4 + x) * 2 + (ca[3] - cb[3]) % 2


def hops(g):
    return sum(min(v, 4 - v) for v in coords(g)[:3])


def make_plan():
    offsets = sorted(OFFSETS, key=lambda a: (hops(a), a))
    n_slots = len(offsets)
    units = [(0, 0, 6, 1), (0, 0, 7, 0)]
    seen = {0}
    for n in range(1, n_slots):
        first = True
        for m in range(n):
            g, back = difference(offsets[n], offsets[m]), difference(offsets[m], offsets[n])
            if g in seen:
                continue
            seen.update((g, back))
            if g == back:
                kinds = (2 + [k for k in range(4) if coords(g)[k]][0],)
            else:
                kinds = (0, 1)
            for kind in kinds:
                units.append((n, m, kind, 1 if first else 0))
                first = False
        assert not first
    assert len(seen) == 128
    while len(units) % UNROLL:
        units.append((0, 0, 6, 0))
    trips = [units[t:t + UNROLL] for t in range(0, len(units), UNROLL)]
    last = {}
    for t, trip in enumerate(trips):
        for i, j, _, _ in trip:
            last[i] = t
            last[j] = t
    finished = sorted(range(1, n_slots), key=lambda slot: (last[slot], slot))
    words = []
    need = 1
    for t, trip in enumerate(trips):
        need = max([need] + [max(i, j) + 1 for i, j, _, _ in trip])
        sent = sum(last[slot] < t for slot in finished)
        codes = [i + 16 * j + 256 * kind for i, j, kind, _ in trip]
        words.append((codes[0] + 2048 * codes[1] + 2 ** 22 * need, codes[2] + 2048 * sent))
    return offsets, finished, words


def pick(values, idx):
    out = jnp.int32(values[0])
    for k in range(1, len(values)):
        out = jnp.where(idx == k, jnp.int32(values[k]), out)
    return out


def wide(a, b):
    return jnp.concatenate([a, b], axis=1)


def kernel(offsets, finished, words, c_ref, s_ref, x_ref, v_ref, out_ref, xs, vts, xl, xt, yt, yrecv, kb, kt,
           xsend, vsend, xrecv, vrecv, ysend, ysem):
    n_slots = len(offsets)
    me = lax.axis_index('group')
    core, px, py, pz = me % 2, (me // 2) % 4, (me // 8) % 4, me // 32
    scale = c_ref[0]
    out_scale = s_ref[0]

    def shifted(z, y, x, c):
        return ((((pz + z) % 4) * 4 + (py + y) % 4) * 4 + (px + x) % 4) * 2 + (core + c) % 2

    def plus(a):
        return shifted(*coords(a))

    def minus(a):
        z, y, x, c = coords(a)
        return shifted((4 - z) % 4, (4 - y) % 4, (4 - x) % 4, c)

    partners = sorted(set(offsets[1:]) | {difference(0, a) for a in offsets[1:]})
    barrier = pltpu.get_barrier_semaphore()
    for a in partners:
        pl.semaphore_signal(barrier, inc=1, device_id=(0, plus(a)), device_id_type=pl.DeviceIdType.MESH)
    pl.semaphore_wait(barrier, len(partners))

    def x_copy(slot, target):
        return pltpu.make_async_remote_copy(
            src_ref=x_ref, dst_ref=xs.at[slot], send_sem=xsend.at[slot], recv_sem=xrecv.at[slot],
            device_id=(0, target), device_id_type=pl.DeviceIdType.MESH)

    def v_copy(slot, target):
        return pltpu.make_async_remote_copy(
            src_ref=v_ref, dst_ref=vts.at[slot], send_sem=vsend.at[slot], recv_sem=vrecv.at[slot],
            device_id=(0, target), device_id_type=pl.DeviceIdType.MESH)

    def y_copy(slot, target):
        return pltpu.make_async_remote_copy(
            src_ref=yt.at[slot], dst_ref=yrecv.at[slot], send_sem=ysend.at[slot], recv_sem=ysem.at[slot],
            device_id=(0, target), device_id_type=pl.DeviceIdType.MESH)

    for slot in range(1, n_slots):
        x_copy(slot, minus(offsets[slot])).start()
        v_copy(slot, minus(offsets[slot])).start()

    xs[0] = x_ref[...]
    vts[0] = v_ref[...]
    kb[...] = jnp.zeros_like(kb)
    kt[...] = jnp.zeros_like(kt)

    def clear(slot, _):
        yt[slot] = jnp.zeros((RHS, ROWS), F32)
        for t in range(ROWS // PANEL):
            xt[lax.min(slot, n_slots - 1), t, FEAT + 16:2 * FEAT, :] = jnp.zeros((FEAT - 16, PANEL), BF16)
        return 0

    lax.fori_loop(0, n_slots + 1, clear, 0)
    row = lax.broadcasted_iota(jnp.int32, (16, PANEL), 0)
    nothing = jnp.zeros((FEAT - 16, PANEL), F32)

    def prepare(slot):
        for t in range(ROWS // PANEL):
            rows = slice(t * PANEL, (t + 1) * PANEL)
            x = xs[slot, rows, :]
            turned = x.T
            xf = turned.astype(F32)
            norm = jnp.sum(xf * xf, axis=0, keepdims=True)
            hi = norm.astype(BF16).astype(F32)
            mid = (norm - hi).astype(BF16).astype(F32)
            low = norm - hi - mid
            three = lambda k: jnp.where(row == k, hi, jnp.where(row == k + 1, mid, low))
            right = jnp.where(row < 3, three(0), jnp.where(row < 6, 1.0, 0.0))
            left = jnp.where(row < 3, 1.0, jnp.where(row < 6, three(3), 0.0))
            xt[slot, t, 0:FEAT, :] = turned
            xt[slot, t, FEAT:FEAT + 16, :] = right.astype(BF16)
            xl[slot, 0, rows, :] = x * BF16(-2.0)
            xl[slot, 1, rows, :] = jnp.concatenate([left, nothing], axis=0).astype(BF16).T

    def arrive(slot, _):
        x_copy(slot, me).wait_recv()
        v_copy(slot, me).wait_recv()
        prepare(slot)
        return 0

    def send_partial(k, _):
        slot = pick(finished, k)
        target = shifted(*(pick([coords(a)[axis] for a in offsets], slot) for axis in range(4)))
        y_copy(slot, target).start()
        return 0

    def decode(code):
        n, m, kind = code % 16, (code // 16) % 16, (code // 256) % 8
        bit = jnp.where(kind == 2, pz // 2, jnp.where(kind == 3, py // 2, jnp.where(kind == 4, px // 2, core)))
        shared = (kind >= 2) & (kind < 6)
        swap = shared & (bit == 1)
        i = jnp.where(swap, m, n)
        j = jnp.where(swap, n, m)
        return i, j, jnp.where(shared, bit, kind % 2), jnp.where(kind >= 6, n_slots, i), j

    parts_i, parts_j = {}, {}

    def add(parts, key, value):
        parts[key] = parts[key] + value if key in parts else value

    def place(step):
        pair, q = divmod(step, 2)
        return 2 * (pair // 3) + q, pair % 3

    def products(step, who):
        i, j, h = who[:3]
        jc, ic = place(step)
        panel = h * 6 + 2 * ic
        add(parts_j, jc, jnp.dot(wide(vts[i, panel], vts[i, panel + 1]), wide(kb[step, 0], kb[step, 1]),
                                 preferred_element_type=F32))
        add(parts_i, ic, jnp.dot(wide(vts[j, 2 * jc], vts[j, 2 * jc + 1]), wide(kt[step, 0], kt[step, 1]),
                                 preferred_element_type=F32))

    def finish_cols(jc, who):
        if jc in parts_j:
            yt[who[4], :, jc * TILE:(jc + 1) * TILE] += parts_j.pop(jc)

    def finish_rows(who):
        for ic in sorted(parts_i):
            cols = pl.ds(pl.multiple_of(who[2] * HALF + ic * TILE, TILE), TILE)
            yt[who[3], :, cols] += parts_i.pop(ic)

    def finish_all(who):
        for jc in sorted(parts_j):
            finish_cols(jc, who)
        finish_rows(who)

    def unit(who, before):
        i, j, h = who[:3]
        for step in range(STEPS):
            jc, ic = place(step)
            rows = pl.ds(pl.multiple_of(h * HALF + ic * TILE, TILE), TILE)
            dist = jnp.dot(wide(xl[i, 0, rows, :], xl[i, 1, rows, :]), wide(xt[j, 2 * jc], xt[j, 2 * jc + 1]),
                           preferred_element_type=F32)
            late = (step - LAG) % STEPS
            owner = who if step >= LAG else before
            products(late, owner)
            if place(late)[1] == 2:
                finish_cols(place(late)[0], owner)
            if step == LAG - 1:
                finish_rows(before)
            kern = (jnp.exp2(jnp.maximum(dist, 0.0) * scale) * out_scale).astype(BF16)
            turned = kern.T
            for e in range(2):
                cols = slice(e * PANEL, (e + 1) * PANEL)
                kb[step, e] = kern[:, cols]
                kt[step, e] = turned[:, cols]

    def trip(t, carry):
        have, sent, before = carry[0], carry[1], carry[2:]
        first, second = pick([w[0] for w in words], t), pick([w[1] for w in words], t)
        need = first // 2 ** 22
        lax.fori_loop(have, need, arrive, 0)
        for code in (first % 2048, (first // 2048) % 2048, second % 2048):
            who = decode(code)
            unit(who, before)
            before = who
        finish_all(before)
        ready = second // 2048
        lax.fori_loop(sent, ready, send_partial, 0)
        return (need, ready) + before

    prepare(0)
    zero = jnp.int32(0)
    carry = lax.fori_loop(0, len(words), trip, (zero + 1, zero, zero, zero, zero, zero + n_slots, zero + n_slots))
    for step in range(STEPS - LAG, STEPS):
        products(step, carry[2:])
    finish_all(carry[2:])
    lax.fori_loop(carry[1], n_slots - 1, send_partial, 0)

    out_ref[...] = yt[0]
    for slot in range(1, n_slots):
        y_copy(slot, me).wait_recv()
        out_ref[...] += yrecv[slot]
    for slot in range(1, n_slots):
        x_copy(slot, me).wait_send()
        v_copy(slot, me).wait_send()
        y_copy(slot, me).wait_send()


def solution(mesh):
    row_spec = P(('tasks', 'group'), None)
    offsets, finished, words = make_plan()
    n_slots = len(offsets)

    def local_fn(x_loc, v_loc, lengthscale, outscale):
        scale = -1.4426950408889634 / (2.0 * jnp.square(lengthscale))
        smem = pl.BlockSpec(memory_space=pltpu.SMEM)
        vmem = pl.BlockSpec(memory_space=pltpu.VMEM)
        dma = pltpu.SemaphoreType.DMA((n_slots,))
        y_t = pl.pallas_call(
            functools.partial(kernel, offsets, finished, words),
            out_shape=jax.ShapeDtypeStruct((RHS, ROWS), F32),
            in_specs=[smem, smem, vmem, vmem],
            out_specs=vmem,
            scratch_shapes=[
                pltpu.VMEM((n_slots, ROWS, FEAT), BF16),
                pltpu.VMEM((n_slots, ROWS // PANEL, RHS, PANEL), BF16),
                pltpu.VMEM((n_slots, 2, ROWS, FEAT), BF16),
                pltpu.VMEM((n_slots, ROWS // PANEL, 2 * FEAT, PANEL), BF16),
                pltpu.VMEM((n_slots + 1, RHS, ROWS), F32),
                pltpu.VMEM((n_slots, RHS, ROWS), F32),
                pltpu.VMEM((STEPS, 2, TILE, PANEL), BF16),
                pltpu.VMEM((STEPS, 2, TILE, PANEL), BF16),
                dma, dma, dma, dma, dma, dma,
            ],
            compiler_params=pltpu.CompilerParams(
                collective_id=0, has_side_effects=True, vmem_limit_bytes=60 * 1024 * 1024),
        )(scale, outscale, x_loc, v_loc.reshape(ROWS // PANEL, PANEL, RHS).transpose(0, 2, 1))
        return y_t.T

    return jax.shard_map(local_fn, mesh=mesh, in_specs=(row_spec, row_spec, P(None), P(None)),
                         out_specs=row_spec, check_vma=False)
```

```python
import functools

import jax
import jax.numpy as jnp
from jax import lax
from jax.experimental import pallas as pl
from jax.experimental.pallas import tpu as pltpu
from jax.sharding import PartitionSpec as P

OFFSETS = (0, 2, 6, 7, 18, 24, 25, 44, 65, 66, 82, 96, 113, 125)
PAIRS = ((1, 0), (2, 1), (3, 1), (3, 0), (3, 2), (4, 3), (4, 0), (4, 1), (5, 0), (5, 1),
         (6, 1), (6, 5), (7, 4), (7, 0), (8, 2), (8, 1), (8, 4), (9, 3), (9, 8), (9, 2),
         (9, 4), (10, 6), (10, 0), (11, 4), (10, 7), (12, 6), (12, 2), (13, 3), (12, 5), (13, 4),
         (12, 0), (10, 5), (11, 5), (12, 10), (10, 4), (13, 5), (9, 5), (9, 1), (8, 7), (12, 11),
         (12, 8), (13, 2), (10, 1), (13, 7), (9, 0), (11, 9), (11, 7), (8, 3), (12, 1), (10, 2),
         (12, 9), (11, 8), (7, 6), (6, 4), (7, 5), (13, 6), (12, 4), (8, 6), (11, 1), (7, 1),
         (12, 7), (9, 6), (10, 8), (13, 0), (8, 0), (13, 10), (13, 11), (11, 10), (6, 0), (11, 6),
         (11, 0))
ROWS = 1536
HALF = 768
UNROLL = 3
LAG = 8
STEPS = 18
PANEL = 128
TILE = 256
FEAT = 128
RHS = 64
F32 = jnp.float32
BF16 = jnp.bfloat16


def coords(g):
    return (g // 32, (g // 8) % 4, (g // 2) % 4, g % 2)


def difference(a, b):
    ca, cb = coords(a), coords(b)
    z, y, x = ((ca[k] - cb[k]) % 4 for k in range(3))
    return ((z * 4 + y) * 4 + x) * 2 + (ca[3] - cb[3]) % 2


def hops(g):
    return sum(min(v, 4 - v) for v in coords(g)[:3])


def make_plan():
    offsets = sorted(OFFSETS, key=lambda a: (hops(a), a))
    n_slots = len(offsets)
    units = [(0, 0, 6), (0, 0, 7)]
    seen = {0}
    for n, m in PAIRS:
        g, back = difference(offsets[n], offsets[m]), difference(offsets[m], offsets[n])
        assert g not in seen
        seen.update((g, back))
        if g == back:
            units.append((n, m, 2 + [k for k in range(4) if coords(g)[k]][0]))
        else:
            units += [(n, m, 0), (n, m, 1)]
    assert len(seen) == 128
    while len(units) % UNROLL:
        units.append((0, 0, 6))
    trips = [units[t:t + UNROLL] for t in range(0, len(units), UNROLL)]
    last = {}
    for t, trip in enumerate(trips):
        for i, j, _ in trip:
            last[i] = t
            last[j] = t
    finished = sorted(range(1, n_slots), key=lambda slot: (last[slot], slot))
    words = []
    need = 1
    for t, trip in enumerate(trips):
        need = max([need] + [max(i, j) + 1 for i, j, _ in trip])
        sent = sum(last[slot] < t for slot in finished)
        codes = [i + 16 * j + 256 * kind for i, j, kind in trip]
        words.append((codes[0] + 2048 * codes[1] + 2 ** 22 * need, codes[2] + 2048 * sent))
    return offsets, finished, words


def pick(values, idx):
    out = jnp.int32(values[0])
    for k in range(1, len(values)):
        out = jnp.where(idx == k, jnp.int32(values[k]), out)
    return out


def wide(a, b):
    return jnp.concatenate([a, b], axis=1)


def kernel(offsets, finished, words, c_ref, s_ref, x_ref, v_ref, out_ref, xs, vts, xl, xt, yt, yrecv, kb, kt,
           xsend, vsend, xrecv, vrecv, ysend, ysem):
    n_slots = len(offsets)
    me = lax.axis_index('group')
    core, px, py, pz = me % 2, (me // 2) % 4, (me // 8) % 4, me // 32
    scale = c_ref[0]
    out_scale = s_ref[0]

    def shifted(z, y, x, c):
        return ((((pz + z) % 4) * 4 + (py + y) % 4) * 4 + (px + x) % 4) * 2 + (core + c) % 2

    def plus(a):
        return shifted(*coords(a))

    def minus(a):
        z, y, x, c = coords(a)
        return shifted((4 - z) % 4, (4 - y) % 4, (4 - x) % 4, c)

    partners = sorted(set(offsets[1:]) | {difference(0, a) for a in offsets[1:]})
    barrier = pltpu.get_barrier_semaphore()
    for a in partners:
        pl.semaphore_signal(barrier, inc=1, device_id=(0, plus(a)), device_id_type=pl.DeviceIdType.MESH)
    pl.semaphore_wait(barrier, len(partners))

    def x_copy(slot, target):
        return pltpu.make_async_remote_copy(
            src_ref=x_ref, dst_ref=xs.at[slot], send_sem=xsend.at[slot], recv_sem=xrecv.at[slot],
            device_id=(0, target), device_id_type=pl.DeviceIdType.MESH)

    def v_copy(slot, target):
        return pltpu.make_async_remote_copy(
            src_ref=v_ref, dst_ref=vts.at[slot], send_sem=vsend.at[slot], recv_sem=vrecv.at[slot],
            device_id=(0, target), device_id_type=pl.DeviceIdType.MESH)

    def y_copy(slot, target):
        return pltpu.make_async_remote_copy(
            src_ref=yt.at[slot], dst_ref=yrecv.at[slot], send_sem=ysend.at[slot], recv_sem=ysem.at[slot],
            device_id=(0, target), device_id_type=pl.DeviceIdType.MESH)

    for slot in range(1, n_slots):
        x_copy(slot, minus(offsets[slot])).start()
        v_copy(slot, minus(offsets[slot])).start()

    xs[0] = x_ref[...]
    vts[0] = v_ref[...]
    kb[...] = jnp.zeros_like(kb)
    kt[...] = jnp.zeros_like(kt)

    def clear(slot, _):
        yt[slot] = jnp.zeros((RHS, ROWS), F32)
        for t in range(ROWS // PANEL):
            xt[lax.min(slot, n_slots - 1), t, FEAT + 16:2 * FEAT, :] = jnp.zeros((FEAT - 16, PANEL), BF16)
        return 0

    lax.fori_loop(0, n_slots + 1, clear, 0)
    row = lax.broadcasted_iota(jnp.int32, (16, PANEL), 0)
    nothing = jnp.zeros((FEAT - 16, PANEL), F32)

    def prepare(slot):
        for t in range(ROWS // PANEL):
            rows = slice(t * PANEL, (t + 1) * PANEL)
            x = xs[slot, rows, :]
            turned = x.T
            xf = turned.astype(F32)
            norm = jnp.sum(xf * xf, axis=0, keepdims=True)
            hi = norm.astype(BF16).astype(F32)
            mid = (norm - hi).astype(BF16).astype(F32)
            low = norm - hi - mid
            three = lambda k: jnp.where(row == k, hi, jnp.where(row == k + 1, mid, low))
            right = jnp.where(row < 3, three(0), jnp.where(row < 6, 1.0, 0.0))
            left = jnp.where(row < 3, 1.0, jnp.where(row < 6, three(3), 0.0))
            xt[slot, t, 0:FEAT, :] = turned
            xt[slot, t, FEAT:FEAT + 16, :] = right.astype(BF16)
            xl[slot, 0, rows, :] = x * BF16(-2.0)
            xl[slot, 1, rows, :] = jnp.concatenate([left, nothing], axis=0).astype(BF16).T

    def arrive(slot, _):
        x_copy(slot, me).wait_recv()
        v_copy(slot, me).wait_recv()
        prepare(slot)
        return 0

    def send_partial(k, _):
        slot = pick(finished, k)
        target = shifted(*(pick([coords(a)[axis] for a in offsets], slot) for axis in range(4)))
        y_copy(slot, target).start()
        return 0

    def decode(code):
        n, m, kind = code % 16, (code // 16) % 16, (code // 256) % 8
        bit = jnp.where(kind == 2, pz // 2, jnp.where(kind == 3, py // 2, jnp.where(kind == 4, px // 2, core)))
        shared = (kind >= 2) & (kind < 6)
        swap = shared & (bit == 1)
        i = jnp.where(swap, m, n)
        j = jnp.where(swap, n, m)
        return i, j, jnp.where(shared, bit, kind % 2), jnp.where(kind >= 6, n_slots, i), j

    parts_i, parts_j = {}, {}

    def add(parts, key, value):
        parts[key] = parts[key] + value if key in parts else value

    def place(step):
        pair, q = divmod(step, 2)
        return 2 * (pair // 3) + q, pair % 3

    def products(step, who):
        i, j, h = who[:3]
        jc, ic = place(step)
        panel = h * 6 + 2 * ic
        add(parts_j, jc, jnp.dot(wide(vts[i, panel], vts[i, panel + 1]), wide(kb[step, 0], kb[step, 1]),
                                 preferred_element_type=F32))
        add(parts_i, ic, jnp.dot(wide(vts[j, 2 * jc], vts[j, 2 * jc + 1]), wide(kt[step, 0], kt[step, 1]),
                                 preferred_element_type=F32))

    def finish_cols(jc, who):
        if jc in parts_j:
            yt[who[4], :, jc * TILE:(jc + 1) * TILE] += parts_j.pop(jc)

    def finish_rows(who):
        for ic in sorted(parts_i):
            cols = pl.ds(pl.multiple_of(who[2] * HALF + ic * TILE, TILE), TILE)
            yt[who[3], :, cols] += parts_i.pop(ic)

    def finish_all(who):
        for jc in sorted(parts_j):
            finish_cols(jc, who)
        finish_rows(who)

    def unit(who, before):
        i, j, h = who[:3]
        for step in range(STEPS):
            jc, ic = place(step)
            rows = pl.ds(pl.multiple_of(h * HALF + ic * TILE, TILE), TILE)
            dist = jnp.dot(wide(xl[i, 0, rows, :], xl[i, 1, rows, :]), wide(xt[j, 2 * jc], xt[j, 2 * jc + 1]),
                           preferred_element_type=F32)
            late = (step - LAG) % STEPS
            owner = who if step >= LAG else before
            products(late, owner)
            if place(late)[1] == 2:
                finish_cols(place(late)[0], owner)
            if step == LAG - 1:
                finish_rows(before)
            kern = (jnp.exp2(jnp.maximum(dist, 0.0) * scale) * out_scale).astype(BF16)
            turned = kern.T
            for e in range(2):
                cols = slice(e * PANEL, (e + 1) * PANEL)
                kb[step, e] = kern[:, cols]
                kt[step, e] = turned[:, cols]

    def trip(t, carry):
        have, sent, before = carry[0], carry[1], carry[2:]
        first, second = pick([w[0] for w in words], t), pick([w[1] for w in words], t)
        need = first // 2 ** 22
        lax.fori_loop(have, need, arrive, 0)
        for code in (first % 2048, (first // 2048) % 2048, second % 2048):
            who = decode(code)
            unit(who, before)
            before = who
        finish_all(before)
        ready = second // 2048
        lax.fori_loop(sent, ready, send_partial, 0)
        return (need, ready) + before

    prepare(0)
    zero = jnp.int32(0)
    carry = lax.fori_loop(0, len(words), trip, (zero + 1, zero, zero, zero, zero, zero + n_slots, zero + n_slots))
    for step in range(STEPS - LAG, STEPS):
        products(step, carry[2:])
    finish_all(carry[2:])
    lax.fori_loop(carry[1], n_slots - 1, send_partial, 0)

    out_ref[...] = yt[0]
    for slot in range(1, n_slots):
        y_copy(slot, me).wait_recv()
        out_ref[...] += yrecv[slot]
    for slot in range(1, n_slots):
        x_copy(slot, me).wait_send()
        v_copy(slot, me).wait_send()
        y_copy(slot, me).wait_send()


def solution(mesh):
    row_spec = P(('tasks', 'group'), None)
    offsets, finished, words = make_plan()
    n_slots = len(offsets)

    def local_fn(x_loc, v_loc, lengthscale, outscale):
        scale = -1.4426950408889634 / (2.0 * jnp.square(lengthscale))
        smem = pl.BlockSpec(memory_space=pltpu.SMEM)
        vmem = pl.BlockSpec(memory_space=pltpu.VMEM)
        dma = pltpu.SemaphoreType.DMA((n_slots,))
        y_t = pl.pallas_call(
            functools.partial(kernel, offsets, finished, words),
            out_shape=jax.ShapeDtypeStruct((RHS, ROWS), F32),
            in_specs=[smem, smem, vmem, vmem],
            out_specs=vmem,
            scratch_shapes=[
                pltpu.VMEM((n_slots, ROWS, FEAT), BF16),
                pltpu.VMEM((n_slots, ROWS // PANEL, RHS, PANEL), BF16),
                pltpu.VMEM((n_slots, 2, ROWS, FEAT), BF16),
                pltpu.VMEM((n_slots, ROWS // PANEL, 2 * FEAT, PANEL), BF16),
                pltpu.VMEM((n_slots + 1, RHS, ROWS), F32),
                pltpu.VMEM((n_slots, RHS, ROWS), F32),
                pltpu.VMEM((STEPS, 2, TILE, PANEL), BF16),
                pltpu.VMEM((STEPS, 2, TILE, PANEL), BF16),
                dma, dma, dma, dma, dma, dma,
            ],
            compiler_params=pltpu.CompilerParams(
                collective_id=0, has_side_effects=True, vmem_limit_bytes=60 * 1024 * 1024),
        )(scale, outscale, x_loc, v_loc.reshape(ROWS // PANEL, PANEL, RHS).transpose(0, 2, 1))
        return y_t.T

    return jax.shard_map(local_fn, mesh=mesh, in_specs=(row_spec, row_spec, P(None), P(None)),
                         out_specs=row_spec, check_vma=False)
```

```python
import functools

import jax
import jax.numpy as jnp
from jax import lax
from jax.experimental import pallas as pl
from jax.experimental.pallas import tpu as pltpu
from jax.sharding import PartitionSpec as P

OFFSETS = (0, 2, 6, 7, 18, 24, 25, 44, 65, 66, 82, 96, 113, 125)
PAIRS = ((2, 1), (2, 0), (3, 2), (3, 1), (3, 0), (4, 3), (4, 1), (4, 0), (5, 1), (5, 3),
         (6, 4), (6, 1), (7, 4), (7, 0), (7, 6), (8, 6), (8, 2), (8, 1), (8, 3), (9, 3),
         (9, 2), (9, 4), (10, 6), (10, 7), (10, 4), (11, 4), (11, 2), (11, 10), (12, 11), (12, 4),
         (13, 5), (12, 5), (12, 8), (13, 3), (13, 2), (13, 8), (13, 6), (13, 4), (11, 9), (12, 6),
         (11, 3), (13, 7), (10, 2), (12, 7), (13, 12), (12, 0), (7, 5), (13, 0), (11, 1), (10, 5),
         (10, 1), (8, 0), (7, 1), (12, 9), (12, 10), (11, 7), (7, 3), (9, 5), (8, 7), (11, 8),
         (13, 10), (10, 8), (9, 8), (10, 0), (11, 6), (9, 6), (6, 0), (6, 5), (11, 5), (5, 0),
         (11, 0))
ROWS = 1536
HALF = 768
UNROLL = 3
LAG = 8
STEPS = 18
PANEL = 128
TILE = 256
FEAT = 128
RHS = 64
F32 = jnp.float32
BF16 = jnp.bfloat16


def coords(g):
    return (g // 32, (g // 8) % 4, (g // 2) % 4, g % 2)


def difference(a, b):
    ca, cb = coords(a), coords(b)
    z, y, x = ((ca[k] - cb[k]) % 4 for k in range(3))
    return ((z * 4 + y) * 4 + x) * 2 + (ca[3] - cb[3]) % 2


def hops(g):
    return sum(min(v, 4 - v) for v in coords(g)[:3])


def make_plan():
    offsets = sorted(OFFSETS, key=lambda a: (hops(a), a))
    n_slots = len(offsets)
    units = [(0, 0, 6), (0, 0, 7)]
    seen = {0}
    for n, m in PAIRS:
        g, back = difference(offsets[n], offsets[m]), difference(offsets[m], offsets[n])
        assert g not in seen
        seen.update((g, back))
        if g == back:
            units.append((n, m, 2 + [k for k in range(4) if coords(g)[k]][0]))
        else:
            units += [(n, m, 0), (n, m, 1)]
    assert len(seen) == 128
    while len(units) % UNROLL:
        units.append((0, 0, 6))
    trips = [units[t:t + UNROLL] for t in range(0, len(units), UNROLL)]
    last = {}
    for t, trip in enumerate(trips):
        for i, j, _ in trip:
            last[i] = t
            last[j] = t
    finished = sorted(range(1, n_slots), key=lambda slot: (last[slot], slot))
    words = []
    need = 1
    for t, trip in enumerate(trips):
        need = max([need] + [max(i, j) + 1 for i, j, _ in trip])
        sent = sum(last[slot] < t for slot in finished)
        codes = [i + 16 * j + 256 * kind for i, j, kind in trip]
        words.append((codes[0] + 2048 * codes[1] + 2 ** 22 * need, codes[2] + 2048 * sent))
    return offsets, finished, words


def pick(values, idx):
    out = jnp.int32(values[0])
    for k in range(1, len(values)):
        out = jnp.where(idx == k, jnp.int32(values[k]), out)
    return out


def wide(a, b):
    return jnp.concatenate([a, b], axis=1)


def kernel(offsets, finished, words, c_ref, s_ref, x_ref, v_ref, out_ref, xs, vts, xl, xt, yt, yrecv, kb, kt,
           xsend, vsend, xrecv, vrecv, ysend, ysem):
    n_slots = len(offsets)
    me = lax.axis_index('group')
    core, px, py, pz = me % 2, (me // 2) % 4, (me // 8) % 4, me // 32
    scale = c_ref[0]
    out_scale = s_ref[0]

    def shifted(z, y, x, c):
        return ((((pz + z) % 4) * 4 + (py + y) % 4) * 4 + (px + x) % 4) * 2 + (core + c) % 2

    def plus(a):
        return shifted(*coords(a))

    def minus(a):
        z, y, x, c = coords(a)
        return shifted((4 - z) % 4, (4 - y) % 4, (4 - x) % 4, c)

    partners = sorted(set(offsets[1:]) | {difference(0, a) for a in offsets[1:]})
    barrier = pltpu.get_barrier_semaphore()
    for a in partners:
        pl.semaphore_signal(barrier, inc=1, device_id=(0, plus(a)), device_id_type=pl.DeviceIdType.MESH)
    pl.semaphore_wait(barrier, len(partners))

    def x_copy(slot, target):
        return pltpu.make_async_remote_copy(
            src_ref=x_ref, dst_ref=xs.at[slot], send_sem=xsend.at[slot], recv_sem=xrecv.at[slot],
            device_id=(0, target), device_id_type=pl.DeviceIdType.MESH)

    def v_copy(slot, target):
        return pltpu.make_async_remote_copy(
            src_ref=v_ref, dst_ref=vts.at[slot], send_sem=vsend.at[slot], recv_sem=vrecv.at[slot],
            device_id=(0, target), device_id_type=pl.DeviceIdType.MESH)

    def y_copy(slot, target):
        return pltpu.make_async_remote_copy(
            src_ref=yt.at[slot], dst_ref=yrecv.at[slot], send_sem=ysend.at[slot], recv_sem=ysem.at[slot],
            device_id=(0, target), device_id_type=pl.DeviceIdType.MESH)

    for slot in range(1, n_slots):
        x_copy(slot, minus(offsets[slot])).start()
        v_copy(slot, minus(offsets[slot])).start()

    xs[0] = x_ref[...]
    vts[0] = v_ref[...]
    kb[...] = jnp.zeros_like(kb)
    kt[...] = jnp.zeros_like(kt)

    def clear(slot, _):
        yt[slot] = jnp.zeros((RHS, ROWS), F32)
        for t in range(ROWS // PANEL):
            xt[lax.min(slot, n_slots - 1), t, FEAT + 16:2 * FEAT, :] = jnp.zeros((FEAT - 16, PANEL), BF16)
        return 0

    lax.fori_loop(0, n_slots + 1, clear, 0)
    row = lax.broadcasted_iota(jnp.int32, (16, PANEL), 0)
    nothing = jnp.zeros((FEAT - 16, PANEL), F32)

    def prepare(slot):
        for t in range(ROWS // PANEL):
            rows = slice(t * PANEL, (t + 1) * PANEL)
            x = xs[slot, rows, :]
            turned = x.T
            xf = turned.astype(F32)
            norm = jnp.sum(xf * xf, axis=0, keepdims=True)
            hi = norm.astype(BF16).astype(F32)
            mid = (norm - hi).astype(BF16).astype(F32)
            low = norm - hi - mid
            three = lambda k: jnp.where(row == k, hi, jnp.where(row == k + 1, mid, low))
            right = jnp.where(row < 3, three(0), jnp.where(row < 6, 1.0, 0.0))
            left = jnp.where(row < 3, 1.0, jnp.where(row < 6, three(3), 0.0))
            xt[slot, t, 0:FEAT, :] = turned
            xt[slot, t, FEAT:FEAT + 16, :] = right.astype(BF16)
            xl[slot, 0, rows, :] = x * BF16(-2.0)
            xl[slot, 1, rows, :] = jnp.concatenate([left, nothing], axis=0).astype(BF16).T

    def arrive(slot, _):
        x_copy(slot, me).wait_recv()
        v_copy(slot, me).wait_recv()
        prepare(slot)
        return 0

    def send_partial(k, _):
        slot = pick(finished, k)
        target = shifted(*(pick([coords(a)[axis] for a in offsets], slot) for axis in range(4)))
        y_copy(slot, target).start()
        return 0

    def decode(code):
        n, m, kind = code % 16, (code // 16) % 16, (code // 256) % 8
        bit = jnp.where(kind == 2, pz // 2, jnp.where(kind == 3, py // 2, jnp.where(kind == 4, px // 2, core)))
        shared = (kind >= 2) & (kind < 6)
        swap = shared & (bit == 1)
        i = jnp.where(swap, m, n)
        j = jnp.where(swap, n, m)
        return i, j, jnp.where(shared, bit, kind % 2), jnp.where(kind >= 6, n_slots, i), j

    parts_i, parts_j = {}, {}

    def add(parts, key, value):
        parts[key] = parts[key] + value if key in parts else value

    def place(step):
        pair, q = divmod(step, 2)
        return 2 * (pair // 3) + q, pair % 3

    def products(step, who):
        i, j, h = who[:3]
        jc, ic = place(step)
        panel = h * 6 + 2 * ic
        add(parts_j, jc, jnp.dot(wide(vts[i, panel], vts[i, panel + 1]), wide(kb[step, 0], kb[step, 1]),
                                 preferred_element_type=F32))
        add(parts_i, ic, jnp.dot(wide(vts[j, 2 * jc], vts[j, 2 * jc + 1]), wide(kt[step, 0], kt[step, 1]),
                                 preferred_element_type=F32))

    def finish_cols(jc, who):
        if jc in parts_j:
            yt[who[4], :, jc * TILE:(jc + 1) * TILE] += parts_j.pop(jc)

    def finish_rows(who):
        for ic in sorted(parts_i):
            cols = pl.ds(pl.multiple_of(who[2] * HALF + ic * TILE, TILE), TILE)
            yt[who[3], :, cols] += parts_i.pop(ic)

    def finish_all(who):
        for jc in sorted(parts_j):
            finish_cols(jc, who)
        finish_rows(who)

    def unit(who, before):
        i, j, h = who[:3]
        for step in range(STEPS):
            jc, ic = place(step)
            rows = pl.ds(pl.multiple_of(h * HALF + ic * TILE, TILE), TILE)
            dist = jnp.dot(wide(xl[i, 0, rows, :], xl[i, 1, rows, :]), wide(xt[j, 2 * jc], xt[j, 2 * jc + 1]),
                           preferred_element_type=F32)
            late = (step - LAG) % STEPS
            owner = who if step >= LAG else before
            products(late, owner)
            if place(late)[1] == 2:
                finish_cols(place(late)[0], owner)
            if step == LAG - 1:
                finish_rows(before)
            kern = (jnp.exp2(jnp.maximum(dist, 0.0) * scale) * out_scale).astype(BF16)
            turned = kern.T
            for e in range(2):
                cols = slice(e * PANEL, (e + 1) * PANEL)
                kb[step, e] = kern[:, cols]
                kt[step, e] = turned[:, cols]

    def trip(t, carry):
        have, sent, before = carry[0], carry[1], carry[2:]
        first, second = pick([w[0] for w in words], t), pick([w[1] for w in words], t)
        need = first // 2 ** 22
        lax.fori_loop(have, need, arrive, 0)
        for code in (first % 2048, (first // 2048) % 2048, second % 2048):
            who = decode(code)
            unit(who, before)
            before = who
        finish_all(before)
        ready = second // 2048
        lax.fori_loop(sent, ready, send_partial, 0)
        return (need, ready) + before

    prepare(0)
    zero = jnp.int32(0)
    carry = lax.fori_loop(0, len(words), trip, (zero + 1, zero, zero, zero, zero, zero + n_slots, zero + n_slots))
    for step in range(STEPS - LAG, STEPS):
        products(step, carry[2:])
    finish_all(carry[2:])
    lax.fori_loop(carry[1], n_slots - 1, send_partial, 0)

    out_ref[...] = yt[0]
    for slot in finished:
        y_copy(slot, me).wait_recv()
        out_ref[...] += yrecv[slot]
    for slot in range(1, n_slots):
        x_copy(slot, me).wait_send()
        v_copy(slot, me).wait_send()
        y_copy(slot, me).wait_send()


def solution(mesh):
    row_spec = P(('tasks', 'group'), None)
    offsets, finished, words = make_plan()
    n_slots = len(offsets)

    def local_fn(x_loc, v_loc, lengthscale, outscale):
        scale = -1.4426950408889634 / (2.0 * jnp.square(lengthscale))
        smem = pl.BlockSpec(memory_space=pltpu.SMEM)
        vmem = pl.BlockSpec(memory_space=pltpu.VMEM)
        dma = pltpu.SemaphoreType.DMA((n_slots,))
        y_t = pl.pallas_call(
            functools.partial(kernel, offsets, finished, words),
            out_shape=jax.ShapeDtypeStruct((RHS, ROWS), F32),
            in_specs=[smem, smem, vmem, vmem],
            out_specs=vmem,
            scratch_shapes=[
                pltpu.VMEM((n_slots, ROWS, FEAT), BF16),
                pltpu.VMEM((n_slots, ROWS // PANEL, RHS, PANEL), BF16),
                pltpu.VMEM((n_slots, 2, ROWS, FEAT), BF16),
                pltpu.VMEM((n_slots, ROWS // PANEL, 2 * FEAT, PANEL), BF16),
                pltpu.VMEM((n_slots + 1, RHS, ROWS), F32),
                pltpu.VMEM((n_slots, RHS, ROWS), F32),
                pltpu.VMEM((STEPS, 2, TILE, PANEL), BF16),
                pltpu.VMEM((STEPS, 2, TILE, PANEL), BF16),
                dma, dma, dma, dma, dma, dma,
            ],
            compiler_params=pltpu.CompilerParams(
                collective_id=0, has_side_effects=True, vmem_limit_bytes=60 * 1024 * 1024),
        )(scale, outscale, x_loc, v_loc.reshape(ROWS // PANEL, PANEL, RHS).transpose(0, 2, 1))
        return y_t.T

    return jax.shard_map(local_fn, mesh=mesh, in_specs=(row_spec, row_spec, P(None), P(None)),
                         out_specs=row_spec, check_vma=False)
```
